128 devices in a mesh: replica: 1, heads: 16 (over z, y), model: 8 (over x, core).
Axes of the slice: x: 4, y: 4, z: 4, core: 2. Of those that a mesh axis runs over, the one named last changes fastest.
Arguments:
- tokens: bfloat16 [512, 8192], P('replica')
- w_query: bfloat16 [8192, 8192], P(None, ('heads', 'model'))
- w_key: bfloat16 [8192, 512], replicated
- w_value: bfloat16 [8192, 512], replicated
- w_out: bfloat16 [8192, 8192], P(('heads', 'model'))
- key_cache: bfloat16 [512, 8, 1024, 64], P(('replica', 'model'))
- value_cache: bfloat16 [512, 8, 1024, 64], P(('replica', 'model'))
- lengths: int32 [512], P(('replica', 'model'))
Outputs:
- output 1: bfloat16 [512, 8192], P('replica')
- output 2: bfloat16 [512, 8, 64], P(('replica', 'model'))
- output 3: bfloat16 [512, 8, 64], P(('replica', 'model'))
All inputs are finite; a program needn't handle non-finite values.
Results may differ from the reference program's by a relative error of at most 0.00223736.
Values are sent between devices in bfloat16 or wider.
A program may use at most 1 GiB of HBM per device.

```python
import jax
import jax.numpy as jnp
from jax import lax

D = 8192
QHEADS = 128
KVHEADS = 8
HEAD = 64
BATCH = 512
CONTEXT = 1024
GROUP_SIZE = QHEADS // KVHEADS
SCALE = HEAD ** -0.5


def draw_lengths(len_key):
    len_keys = jax.random.split(len_key, 2)
    lengths = jax.random.randint(len_keys[0], (BATCH,), 1, CONTEXT, dtype=jnp.int32)
    perm_order = jax.random.permutation(len_keys[1], BATCH)
    return lengths.at[perm_order[0]].set(CONTEXT - 1).at[perm_order[1]].set(1)


def setup_inputs(seed: int = 0, part: int = 0) -> dict:
    base_key = jax.random.key(seed)
    part_key = jax.random.fold_in(base_key, part)
    part_keys = jax.random.split(part_key, 3)
    weight_keys = jax.random.split(base_key, 4)
    query_cols = QHEADS * HEAD
    kv_cols = KVHEADS * HEAD
    tokens = jax.random.normal(part_keys[0], (BATCH, D), jnp.float32)
    w_query = jax.random.normal(weight_keys[0], (D, query_cols), jnp.float32) * D ** -0.5
    w_key = jax.random.normal(weight_keys[1], (D, kv_cols), jnp.float32) * (3.0 * D ** -0.5)
    w_value = jax.random.normal(weight_keys[2], (D, kv_cols), jnp.float32) * D ** -0.5
    w_out = jax.random.normal(weight_keys[3], (query_cols, D), jnp.float32) * query_cols ** -0.5
    key_cache = 3.0 * jax.random.normal(part_keys[1], (BATCH, KVHEADS, CONTEXT, HEAD), jnp.float32)
    value_cache = jax.random.normal(part_keys[2], (BATCH, KVHEADS, CONTEXT, HEAD), jnp.float32)
    lengths = draw_lengths(jax.random.fold_in(part_key, 3))
    return {
        "tokens": tokens.astype(jnp.bfloat16),
        "w_query": w_query.astype(jnp.bfloat16),
        "w_key": w_key.astype(jnp.bfloat16),
        "w_value": w_value.astype(jnp.bfloat16),
        "w_out": w_out.astype(jnp.bfloat16),
        "key_cache": key_cache.astype(jnp.bfloat16),
        "value_cache": value_cache.astype(jnp.bfloat16),
        "lengths": lengths,
    }


def reference(tokens, w_query, w_key, w_value, w_out, key_cache, value_cache, lengths):
    queries = jnp.dot(tokens, w_query, preferred_element_type=jnp.float32).astype(jnp.bfloat16)
    queries = queries.reshape(BATCH, KVHEADS, GROUP_SIZE, HEAD)
    key_new = jnp.dot(tokens, w_key, preferred_element_type=jnp.float32).astype(jnp.bfloat16)
    key_new = key_new.reshape(BATCH, KVHEADS, HEAD)
    value_new = jnp.dot(tokens, w_value, preferred_element_type=jnp.float32).astype(jnp.bfloat16)
    value_new = value_new.reshape(BATCH, KVHEADS, HEAD)

    def one_sequence(item):
        q_seq, key_seq, value_seq, key_last, value_last, seq_len = item
        q_wide = q_seq.astype(jnp.float32)
        scores = jnp.einsum("grd,gtd->grt", q_wide, key_seq.astype(jnp.float32)) * SCALE
        score_new = jnp.einsum("grd,gd->gr", q_wide, key_last.astype(jnp.float32)) * SCALE
        positions = jnp.arange(CONTEXT)
        scores = jnp.where(positions < seq_len, scores, -jnp.inf)
        score_max = jnp.maximum(jnp.max(scores, axis=-1), score_new)
        weights = jnp.exp(scores - score_max[..., None])
        weight_new = jnp.exp(score_new - score_max)
        denom_sum = jnp.sum(weights, axis=-1) + weight_new
        weighted_sum = jnp.einsum("grt,gtd->grd", weights.astype(jnp.bfloat16).astype(jnp.float32), value_seq.astype(jnp.float32))
        weighted_sum = weighted_sum + weight_new.astype(jnp.bfloat16).astype(jnp.float32)[..., None] * value_last.astype(jnp.float32)[:, None, :]
        return (weighted_sum / denom_sum[..., None]).astype(jnp.bfloat16)

    attended = lax.map(one_sequence, (queries, key_cache, value_cache, key_new, value_new, lengths))
    mixed_sum = jnp.dot(attended.reshape(BATCH, QHEADS * HEAD), w_out, preferred_element_type=jnp.float32)
    out_tokens = (tokens.astype(jnp.float32) + mixed_sum).astype(jnp.bfloat16)
    return (out_tokens, key_new, value_new)
```

```python
import functools

import jax
import jax.numpy as jnp
from jax import lax
from jax.experimental import pallas as pl
from jax.experimental.pallas import tpu as pltpu
from jax.sharding import PartitionSpec as P

MESH = pl.DeviceIdType.MESH
RING = 4
CHIPS = RING**3
TILE_ROWS, LANES = 16, 128
UNITS = 16
COLOURS = ((0, 5), (5, 10), (10, 16))
ORDERS = (("x", "y", "z"), ("y", "z", "x"), ("z", "x", "y"))
STEPS = (1, 3, 2)
SOURCES = (0, 3, 1, 2)


class Place:
    def __init__(self):
        heads, model = lax.axis_index("heads"), lax.axis_index("model")
        self.at = {"z": heads // RING, "y": heads % RING, "x": model // 2}
        self.core = model % 2

    def device(self, at, core):
        return (0, at["z"] * RING + at["y"], at["x"] * 2 + core)

    def along(self, axis, step):
        at = dict(self.at)
        at[axis] = (at[axis] + step) % RING
        return self.device(at, self.core)

    def sibling(self):
        return self.device(self.at, 1 - self.core)

    def chip(self):
        return (self.at["z"] * RING + self.at["y"]) * RING + self.at["x"]

    def offset(self, n):
        at = {
            "z": (self.at["z"] + n // (RING * RING)) % RING,
            "y": (self.at["y"] + (n // RING) % RING) % RING,
            "x": (self.at["x"] + n % RING) % RING,
        }
        return self.device(at, self.core), (at["z"] * RING + at["y"]) * RING + at["x"]


def remote(src, dst, send_sem, recv_sem, device):
    return pltpu.make_async_remote_copy(
        src_ref=src, dst_ref=dst, send_sem=send_sem, recv_sem=recv_sem, device_id=device, device_id_type=MESH
    )


class Colour:
    def __init__(self, place, held, order, recv, send, share=None):
        self.place, self.held, self.recv, self.send, self.share = place, held, recv, send, share
        self.axes = order
        self.a, self.b, self.c = (place.at[axis] for axis in order)

    def piece(self, row, n):
        return self.held.at[self.c, (self.b + row) % RING, (self.a + n) % RING]

    def row(self, plane, n):
        return self.held.at[(self.c + plane) % RING, (self.b + n) % RING]

    def copy(self, ref, phase, slot, n, step):
        return remote(ref, ref, self.send.at[phase], self.recv.at[phase, slot, n], self.place.along(self.axes[phase], step))

    def wait(self, ref, phase, slot, n):
        self.copy(ref, phase, slot, n, 1).wait_recv()

    def both(self, ref, phase, n):
        self.copy(ref, phase, 0, n, 1).start()
        self.copy(ref, phase, 1, n, 3).start()

    def give(self, ref):
        if self.share is not None:
            remote(ref, ref, self.share.at[0], self.share.at[1], self.place.sibling()).start()

    def open(self):
        own = self.piece(0, 0)
        for slot, step in enumerate(STEPS):
            self.copy(own, 0, slot, 0, step).start()
        self.both(own, 1, 0)

    def line(self, t):
        ref = self.piece(0, SOURCES[t])
        self.wait(ref, 0, t - 1, 0)
        self.both(ref, 1, t)

    def own_row(self):
        self.both(self.row(0, 0), 2, 0)
        self.give(self.row(0, 0))

    def near_pieces(self, t):
        for slot, source, step in ((0, 3, 1), (1, 1, 3)):
            ref = self.piece(source, SOURCES[t])
            self.wait(ref, 1, slot, t)
            if (t in (0, 3)) == (slot == 0):
                self.copy(ref, 1, 2, t, step).start()

    def near_rows(self):
        for n in (1, 2):
            ref = self.row(0, SOURCES[n])
            self.both(ref, 2, n)
            self.give(ref)

    def far_row(self):
        for t in range(RING):
            self.wait(self.piece(2, SOURCES[t]), 1, 2, t)
        self.both(self.row(0, 2), 2, 3)
        self.give(self.row(0, 2))

    def plane_rows(self, n):
        for slot, source, step in ((0, 3, 1), (1, 1, 3)):
            ref = self.row(source, SOURCES[n])
            self.wait(ref, 2, slot, n)
            if (n in (0, 3)) == (slot == 0):
                self.copy(ref, 2, 2, n, step).start()
            self.give(ref)

    def far_plane_row(self, n):
        ref = self.row(2, SOURCES[n])
        self.wait(ref, 2, 2, n)
        self.give(ref)

    def close(self):
        for ref, phase in ((self.held.at[0, 0, 0:3], 0), (self.held.at[0, 0:3], 1), (self.held.at[0:3], 2)):
            remote(ref, ref, self.send.at[phase], self.recv.at[phase, 0, 0], self.place.sibling()).wait_send()

    def close_share(self, other):
        remote(self.held, other, self.share.at[0], self.share.at[1], self.place.sibling()).wait()


def gather(colours):
    for colour in colours:
        colour.open()
    for t in range(1, RING):
        for colour in colours:
            colour.line(t)
    for colour in colours:
        colour.own_row()
    for t in range(RING):
        for colour in colours:
            colour.near_pieces(t)
    for colour in colours:
        colour.near_rows()
    for colour in colours:
        colour.plane_rows(0)
    for colour in colours:
        colour.far_row()
    for n in range(1, RING):
        for colour in colours:
            colour.plane_rows(n)
    for n in range(RING):
        for colour in colours:
            colour.far_plane_row(n)


def project_kernel(
    attended, w_out, tokens, *refs
):
    outs, (heads, w_all, residual, total, recv_in, send_in, recv_out, send_out, share, w_sems, local_sems) = refs[:3], (
        refs[3:6],
        *refs[6:],
    )
    place = Place()
    chip, core = place.chip(), place.core

    barrier = pltpu.get_barrier_semaphore()

    def greet(n, carry):
        device, _ = place.offset(n)
        pl.semaphore_signal(barrier, inc=1, device_id=device, device_id_type=MESH)
        return carry

    lax.fori_loop(1, CHIPS, greet, 0)
    pl.semaphore_signal(barrier, inc=1, device_id=place.sibling(), device_id_type=MESH)

    def own_residual(n):
        rows = pl.ds(pl.multiple_of(n * 128 + core * 64, 64), 64)
        columns = pl.ds(pl.multiple_of(chip * LANES, LANES), LANES)
        return pltpu.make_async_copy(tokens.at[rows, columns], residual.at[pl.ds(n * 64, 64)], local_sems.at[n])

    for n in range(RING):
        own_residual(n).start()

    colours = [
        Colour(place, heads[k], ORDERS[k], recv_in.at[k], send_in.at[k]) for k in range(3)
    ]
    for k, (first, last) in enumerate(COLOURS):
        colour = colours[k]
        for u in range(first, last):
            i, j = u // 4, u % 4
            heads[k][colour.c, colour.b, colour.a, u - first] = attended[
                i * TILE_ROWS : (i + 1) * TILE_ROWS, j * LANES : (j + 1) * LANES
            ]
    own_columns = pl.ds(pl.multiple_of(chip * LANES, LANES), LANES)
    w_all[chip, core] = w_out[:, own_columns]

    pl.semaphore_wait(barrier, CHIPS)

    def send_w(n, carry):
        device, target = place.offset(n)
        columns = pl.ds(pl.multiple_of(target * LANES, LANES), LANES)
        remote(w_out.at[:, columns], w_all.at[chip, core], w_sems.at[0], w_sems.at[1], device).start()
        return carry

    lax.fori_loop(1, CHIPS, send_w, 0)
    gather(colours)

    w_arrived = w_all.at[pl.ds(0, CHIPS - 1), core]
    remote(w_arrived, w_arrived, w_sems.at[0], w_sems.at[1], place.sibling()).wait()
    w_mine, w_theirs = w_all.at[:, core], w_all.at[:, 1 - core]
    remote(w_mine, w_mine, w_sems.at[2], w_sems.at[3], place.sibling()).start()
    remote(w_mine, w_theirs, w_sems.at[2], w_sems.at[3], place.sibling()).wait()

    for n in range(RING):
        own_residual(n).wait()
    total[...] = residual[...].astype(jnp.float32)

    def tile(z, y, x, u):
        k = next(k for k, (first, last) in enumerate(COLOURS) if first <= u < last)
        at = {"z": z, "y": y, "x": x}
        a, b, c = (at[axis] for axis in ORDERS[k])
        return heads[k][c, b, a, u - COLOURS[k][0]]

    def head_step(h, carry):
        z, y = h // RING, h % RING
        rows = [
            jnp.concatenate([tile(z, y, x, i * 4 + j) for j in range(4)], axis=1) for x in range(RING) for i in range(4)
        ]
        lhs = jnp.concatenate(rows, axis=0)
        rhs = w_all[pl.ds(h * RING, RING)].reshape(4 * LANES, LANES)
        total[...] += jnp.dot(lhs, rhs, preferred_element_type=jnp.float32)
        return carry

    lax.fori_loop(0, RING * RING, head_step, 0)

    out_colours = [
        Colour(place, outs[k].at[core], ORDERS[k], recv_out.at[k], send_out.at[k], share.at[k]) for k in range(3)
    ]
    for k, (first, last) in enumerate(COLOURS):
        colour = out_colours[k]
        for u in range(first, last):
            outs[k][core, colour.c, colour.b, colour.a, u - first] = total[
                u * TILE_ROWS : (u + 1) * TILE_ROWS, :
            ].astype(jnp.bfloat16)
    for colour in colours:
        colour.close()
    gather(out_colours)
    for k, colour in enumerate(out_colours):
        colour.close()
        colour.close_share(outs[k].at[1 - core])


def project(attended, w_out, tokens):
    held = [(RING, RING, RING, last - first, TILE_ROWS, LANES) for first, last in COLOURS]
    vmem = pl.BlockSpec(memory_space=pltpu.VMEM)
    return pl.pallas_call(
        project_kernel,
        out_shape=[jax.ShapeDtypeStruct((2, *shape), jnp.bfloat16) for shape in held],
        in_specs=[vmem, vmem, pl.BlockSpec(memory_space=pl.ANY)],
        out_specs=[vmem] * 3,
        scratch_shapes=[pltpu.VMEM(shape, jnp.bfloat16) for shape in held]
        + [
            pltpu.VMEM((CHIPS, 2, 64, LANES), jnp.bfloat16),
            pltpu.VMEM((256, LANES), jnp.bfloat16),
            pltpu.VMEM((256, LANES), jnp.float32),
            pltpu.SemaphoreType.DMA((3, 3, 3, 4)),
            pltpu.SemaphoreType.DMA((3, 3)),
            pltpu.SemaphoreType.DMA((3, 3, 3, 4)),
            pltpu.SemaphoreType.DMA((3, 3)),
            pltpu.SemaphoreType.DMA((3, 2)),
            pltpu.SemaphoreType.DMA((4,)),
            pltpu.SemaphoreType.DMA((4,)),
        ],
        compiler_params=pltpu.CompilerParams(collective_id=0, has_side_effects=True, vmem_limit_bytes=40 << 20),
        name="project_and_gather",
    )(attended, w_out, tokens)


def lay_out_kernel(*refs):
    held, (out, rows, sems) = refs[:3], refs[3:]
    copies = []
    for n in range(RING):
        for core in range(2):
            block = n * 2 + core
            for i in range(4):
                u = n * 4 + i
                k = next(k for k, (first, last) in enumerate(COLOURS) if first <= u < last)
                for chip in range(CHIPS):
                    at = {"z": chip // 16, "y": chip // 4 % 4, "x": chip % 4}
                    a, b, c = (at[axis] for axis in ORDERS[k])
                    rows[block, i * TILE_ROWS : (i + 1) * TILE_ROWS, chip * LANES : (chip + 1) * LANES] = held[k][
                        core, c, b, a, u - COLOURS[k][0]
                    ]
            copy = pltpu.make_async_copy(rows.at[block], out.at[pl.ds(block * 64, 64)], sems.at[block])
            copy.start()
            copies.append(copy)
    for copy in copies:
        copy.wait()


def lay_out(held):
    vmem = pl.BlockSpec(memory_space=pltpu.VMEM)
    return pl.pallas_call(
        lay_out_kernel,
        out_shape=jax.ShapeDtypeStruct((512, CHIPS * LANES), jnp.bfloat16),
        in_specs=[vmem] * 3,
        out_specs=pl.BlockSpec(memory_space=pl.ANY),
        scratch_shapes=[pltpu.VMEM((8, 64, CHIPS * LANES), jnp.bfloat16), pltpu.SemaphoreType.DMA((8,))],
        compiler_params=pltpu.CompilerParams(vmem_limit_bytes=30 << 20),
        name="lay_out",
    )(*held)


def attend(queries, key_rows, value_rows, key_last, value_last, seq_len):
    score_scale = queries.shape[-1] ** -0.5
    scores = jnp.einsum("bgrd,bgtd->bgrt", queries, key_rows, preferred_element_type=jnp.float32) * score_scale
    score_new = jnp.einsum("bgrd,bgd->bgr", queries, key_last, preferred_element_type=jnp.float32) * score_scale
    positions = lax.broadcasted_iota(jnp.int32, (1, 1, 1, key_rows.shape[2]), 3)
    scores = jnp.where(positions < seq_len[:, None, None, None], scores, -jnp.inf)
    score_max = jnp.maximum(jnp.max(scores, axis=-1), score_new)
    weights = jnp.exp(scores - score_max[..., None])
    weight_new = jnp.exp(score_new - score_max)
    denom_sum = jnp.sum(weights, axis=-1) + weight_new
    weighted_sum = jnp.einsum("bgrt,bgtd->bgrd", weights.astype(jnp.bfloat16), value_rows, preferred_element_type=jnp.float32)
    weighted_sum = weighted_sum + weight_new.astype(jnp.bfloat16).astype(jnp.float32)[..., None] * value_last.astype(jnp.float32)[:, :, None, :]
    return (weighted_sum / denom_sum[..., None]).astype(jnp.bfloat16)


def solution(mesh):
    heads_count = mesh.shape["heads"]
    model_count = mesh.shape["model"]

    def local_step(tokens, w_query, w_key, w_value, w_out, key_cache, value_cache, lengths):
        batch_all = tokens.shape[0]
        local_rows = key_cache.shape[0]
        kv_count = key_cache.shape[1]
        head_dim = key_cache.shape[3]
        heads_local = w_query.shape[1] // head_dim
        heads_shard = heads_local * model_count
        group_size = heads_shard * heads_count // kv_count
        shard_groups = max(1, heads_shard // group_size)
        head_index = lax.axis_index("heads")
        model_index = lax.axis_index("model")
        queries = jnp.dot(tokens, w_query, preferred_element_type=jnp.float32).astype(jnp.bfloat16)
        queries = lax.all_to_all(queries.reshape(batch_all, heads_local, head_dim), "model", 0, 1, tiled=True)
        own_tokens = lax.dynamic_slice_in_dim(tokens, model_index * local_rows, local_rows, 0)
        key_new = jnp.dot(own_tokens, w_key, preferred_element_type=jnp.float32).astype(jnp.bfloat16)
        key_new = key_new.reshape(local_rows, kv_count, head_dim)
        value_new = jnp.dot(own_tokens, w_value, preferred_element_type=jnp.float32).astype(jnp.bfloat16)
        value_new = value_new.reshape(local_rows, kv_count, head_dim)
        first_group = head_index * heads_shard // group_size
        attended = attend(
            queries.reshape(local_rows, shard_groups, heads_shard // shard_groups, head_dim),
            lax.dynamic_slice_in_dim(key_cache, first_group, shard_groups, 1),
            lax.dynamic_slice_in_dim(value_cache, first_group, shard_groups, 1),
            lax.dynamic_slice_in_dim(key_new, first_group, shard_groups, 1),
            lax.dynamic_slice_in_dim(value_new, first_group, shard_groups, 1),
            lengths,
        )
        held = project(attended.reshape(local_rows, heads_shard * head_dim), w_out, tokens)
        return (lay_out(held), key_new, value_new)

    cache_spec = P(("replica", "model"), None, None, None)
    new_spec = P(("replica", "model"), None, None)
    return jax.shard_map(
        local_step,
        mesh=mesh,
        in_specs=(P("replica", None), P(None, ("heads", "model")), P(None, None), P(None, None), P(("heads", "model"), None), cache_spec, cache_spec, P(("replica", "model"))),
        out_specs=(P("replica", None), new_spec, new_spec),
        check_vma=False,
    )
```

```python
import functools

import jax
import jax.numpy as jnp
from jax import lax
from jax.experimental import pallas as pl
from jax.experimental.pallas import tpu as pltpu
from jax.sharding import PartitionSpec as P

MESH = pl.DeviceIdType.MESH
RING = 4
CHIPS = RING**3
HEAD = 64
TILE_ROWS, LANES = 16, 128
UNITS = 16
COLOURS = ((0, 6), (6, 10), (10, 16))
ORDERS = (("x", "y", "z"), ("y", "z", "x"), ("z", "x", "y"))
STEPS = (1, 3, 2)
SOURCES = (0, 3, 1, 2)


class Place:
    def __init__(self):
        heads, model = lax.axis_index("heads"), lax.axis_index("model")
        self.at = {"z": heads // RING, "y": heads % RING, "x": model // 2}
        self.core = model % 2

    def device(self, at, core):
        return (0, at["z"] * RING + at["y"], at["x"] * 2 + core)

    def along(self, axis, step):
        at = dict(self.at)
        at[axis] = (at[axis] + step) % RING
        return self.device(at, self.core)

    def sibling(self):
        return self.device(self.at, 1 - self.core)

    def chip(self):
        return (self.at["z"] * RING + self.at["y"]) * RING + self.at["x"]

    def offset(self, n):
        at = {
            "z": (self.at["z"] + n // (RING * RING)) % RING,
            "y": (self.at["y"] + (n // RING) % RING) % RING,
            "x": (self.at["x"] + n % RING) % RING,
        }
        return self.device(at, self.core), (at["z"] * RING + at["y"]) * RING + at["x"]


def remote(src, dst, send_sem, recv_sem, device):
    return pltpu.make_async_remote_copy(
        src_ref=src, dst_ref=dst, send_sem=send_sem, recv_sem=recv_sem, device_id=device, device_id_type=MESH
    )


class Colour:
    def __init__(self, place, held, order, recv, send, share=None):
        self.place, self.held, self.recv, self.send, self.share = place, held, recv, send, share
        self.axes = order
        self.a, self.b, self.c = (place.at[axis] for axis in order)

    def piece(self, row, n):
        return self.held.at[self.c, (self.b + row) % RING, (self.a + n) % RING]

    def row(self, plane, n):
        return self.held.at[(self.c + plane) % RING, (self.b + n) % RING]

    def copy(self, ref, phase, slot, n, step):
        return remote(ref, ref, self.send.at[phase], self.recv.at[phase, slot, n], self.place.along(self.axes[phase], step))

    def wait(self, ref, phase, slot, n):
        self.copy(ref, phase, slot, n, 1).wait_recv()

    def both(self, ref, phase, n):
        self.copy(ref, phase, 0, n, 1).start()
        self.copy(ref, phase, 1, n, 3).start()

    def give(self, ref):
        if self.share is not None:
            remote(ref, ref, self.share.at[0], self.share.at[1], self.place.sibling()).start()

    def open(self):
        own = self.piece(0, 0)
        for slot, step in enumerate(STEPS):
            self.copy(own, 0, slot, 0, step).start()
        self.both(own, 1, 0)

    def line(self, t):
        ref = self.piece(0, SOURCES[t])
        self.wait(ref, 0, t - 1, 0)
        self.both(ref, 1, t)

    def own_row(self):
        self.both(self.row(0, 0), 2, 0)
        self.give(self.row(0, 0))

    def near_pieces(self, t):
        for slot, source, step in ((0, 3, 1), (1, 1, 3)):
            ref = self.piece(source, SOURCES[t])
            self.wait(ref, 1, slot, t)
            if (t in (0, 3)) == (slot == 0):
                self.copy(ref, 1, 2, t, step).start()

    def near_rows(self):
        for n in (1, 2):
            ref = self.row(0, SOURCES[n])
            self.both(ref, 2, n)
            self.give(ref)

    def far_row(self):
        for t in range(RING):
            self.wait(self.piece(2, SOURCES[t]), 1, 2, t)
        self.both(self.row(0, 2), 2, 3)
        self.give(self.row(0, 2))

    def plane_rows(self, n):
        for slot, source, step in ((0, 3, 1), (1, 1, 3)):
            ref = self.row(source, SOURCES[n])
            self.wait(ref, 2, slot, n)
            if (n in (0, 3)) == (slot == 0):
                self.copy(ref, 2, 2, n, step).start()
            self.give(ref)

    def far_plane_row(self, n):
        ref = self.row(2, SOURCES[n])
        self.wait(ref, 2, 2, n)
        self.give(ref)

    def close(self):
        for ref, phase in ((self.held.at[0, 0, 0:3], 0), (self.held.at[0, 0:3], 1), (self.held.at[0:3], 2)):
            remote(ref, ref, self.send.at[phase], self.recv.at[phase, 0, 0], self.place.sibling()).wait_send()

    def close_share(self, other):
        remote(self.held, other, self.share.at[0], self.share.at[1], self.place.sibling()).wait()


def gather(colours, fillers=()):
    fillers = list(fillers)
    steps = [(Colour.open,)]
    steps += [(Colour.line, t) for t in range(1, RING)]
    steps += [(Colour.own_row,)]
    steps += [(Colour.near_pieces, t) for t in range(RING)]
    steps += [(Colour.near_rows,), (Colour.plane_rows, 0), (Colour.far_row,)]
    steps += [(Colour.plane_rows, n) for n in range(1, RING)]
    steps += [(Colour.far_plane_row, n) for n in range(RING)]
    for step, *args in steps:
        for colour in colours:
            step(colour, *args)
        if fillers:
            fillers.pop(0)()
    for filler in fillers:
        filler()


def step_kernel(
    tokens, w_query, w_key, w_value, w_out, key_cache, value_cache, lengths,
    out_a, out_b, out_c, key_new, value_new,
    head_a, head_b, head_c, w_all, tok, wq, w_kv, keys, values, query, by_head, by_seq,
    attended, to_seq, to_head, kv_own, total, residual,
    recv_in, send_in, recv_out, send_out, share, w_sems, q_sems, local_sems,
):
    outs, heads = (out_a, out_b, out_c), (head_a, head_b, head_c)
    place = Place()
    chip, core = place.chip(), place.core
    head_at, model_at = lax.axis_index("heads"), lax.axis_index("model")
    group, half = head_at // 2, head_at % 2
    barrier = pltpu.get_barrier_semaphore()

    def partner(n):
        other_half, other_model = (half + n // 8) % 2, (model_at + n % 8) % 8
        return (0, group * 2 + other_half, other_model), other_half, other_model

    def signal(device):
        pl.semaphore_signal(barrier, inc=1, device_id=device, device_id_type=MESH)

    def greet_chip(n, carry):
        signal(place.offset(n)[0])
        return carry

    lax.fori_loop(1, CHIPS, greet_chip, 0)
    for n in range(RING):
        for other_half in range(2):
            signal((0, group * 2 + other_half, n * 2 + 1 - core))

    def token_copy(n):
        return pltpu.make_async_copy(tokens.at[:, pl.ds(n * 1024, 1024)], tok.at[n], local_sems.at[n])

    wq_copy = pltpu.make_async_copy(w_query, wq, local_sems.at[8])
    wq_copy.start()
    for n in range(8):
        token_copy(n).start()

    def kv_block(n):
        return (group // 2 + n) % 4

    def w_kv_copy(which, n):
        columns = pl.ds(pl.multiple_of(kv_block(n) * LANES, LANES), LANES)
        source = (w_key, w_value)[which]
        return pltpu.make_async_copy(source.at[:, columns], w_kv.at[which, n], local_sems.at[9 + which * 4 + n])

    for which in range(2):
        w_kv_copy(which, 0).start()

    def cache_copy(which, n):
        source, held = ((key_cache, keys), (value_cache, values))[which]
        return pltpu.make_async_copy(
            source.at[pl.ds(half * 32 + n * 8, 8), group], held.at[pl.ds(n * 8, 8)], local_sems.at[17 + which * 4 + n]
        )

    for n in range(4):
        for which in range(2):
            cache_copy(which, n).start()

    def residual_copy(n):
        rows = pl.ds(pl.multiple_of(n * 128 + core * 64, 64), 64)
        columns = pl.ds(pl.multiple_of(chip * LANES, LANES), LANES)
        return pltpu.make_async_copy(tokens.at[rows, columns], residual.at[pl.ds(n * 64, 64)], local_sems.at[25 + n])

    for n in range(RING):
        residual_copy(n).start()
    own_w = pltpu.make_async_copy(
        w_out.at[:, pl.ds(pl.multiple_of(chip * LANES, LANES), LANES)], w_all.at[chip, core], local_sems.at[29]
    )
    own_w.start()
    for n in range(1, 4):
        for which in range(2):
            w_kv_copy(which, n).start()

    wq_copy.wait()
    token_copy(0).wait()
    both_last = (((1,), (1,)), ((), ()))

    def query_part(n):
        return lax.dot_general(tok[n], wq[:, n * 1024 : (n + 1) * 1024], both_last, preferred_element_type=jnp.float32)

    acc = query_part(0)
    for n in range(1, 8):
        token_copy(n).wait()
        acc = acc + query_part(n)
    query[:, 0:HEAD] = acc.astype(jnp.bfloat16)
    query[:, HEAD:LANES] = jnp.zeros((512, HEAD), jnp.bfloat16)

    pl.semaphore_wait(barrier, CHIPS - 1 + 2 * RING)
    slot = half * 8 + model_at

    def query_rows(other_half, other_model):
        return query.at[pl.ds(pl.multiple_of(other_model * 64 + other_half * 32, 32), 32)]

    def send_query(n, carry):
        device, other_half, other_model = partner(n)
        remote(query_rows(other_half, other_model), by_head.at[slot], q_sems.at[0], q_sems.at[1], device).start()
        return carry

    lax.fori_loop(1, 16, send_query, 0)

    def send_w(n, carry):
        device, target = place.offset(n)
        columns = pl.ds(pl.multiple_of(target * LANES, LANES), LANES)
        remote(w_out.at[:, columns], w_all.at[chip, core], w_sems.at[0], w_sems.at[1], device).start()
        return carry

    lax.fori_loop(1, CHIPS, send_w, 0)
    by_head[slot] = query_rows(half, model_at)[...]

    own_rows = pl.ds(pl.multiple_of(model_at * 64, 64), 64)

    def new_block(which, n):
        w_kv_copy(which, n).wait()
        acc = jnp.dot(tok[0, own_rows], w_kv[which, n, 0:1024], preferred_element_type=jnp.float32)
        for k in range(1, 8):
            acc = acc + jnp.dot(
                tok[k, own_rows], w_kv[which, n, k * 1024 : (k + 1) * 1024], preferred_element_type=jnp.float32
            )
        acc = acc.astype(jnp.bfloat16)
        columns = pl.ds(pl.multiple_of(kv_block(n) * LANES, LANES), LANES)
        (key_new, value_new)[which][:, columns] = acc
        if n == 0:
            wide = acc.astype(jnp.float32)
            wide = jnp.where(group % 2 == 0, wide, pltpu.roll(wide, HEAD, 1))
            lanes = lax.broadcasted_iota(jnp.int32, wide.shape, 1)
            kv_own[which] = jnp.where(lanes < HEAD, wide, 0.0)

    for which in range(2):
        new_block(which, 0)

    row = lax.broadcasted_iota(jnp.int32, (512, 512), 0)
    column = lax.broadcasted_iota(jnp.int32, (512, 512), 1)
    to_seq[...] = (column == (row % 16) * 32 + row // 16).astype(jnp.float32).astype(jnp.bfloat16)
    pair_row = lax.broadcasted_iota(jnp.int32, (256, 512), 0)
    pair_column = lax.broadcasted_iota(jnp.int32, (256, 512), 1)
    for parity in range(2):
        source = (pair_row % 32) * 16 + (pair_row // 32) * 2 + parity
        to_head[parity] = (pair_column == source).astype(jnp.float32).astype(jnp.bfloat16)

    arrived = by_head.at[pl.ds(0, 15)]
    remote(arrived, arrived, q_sems.at[0], q_sems.at[1], place.sibling()).wait()
    by_seq[...] = jnp.dot(
        to_seq[...], by_head[...].reshape(512, LANES), preferred_element_type=jnp.float32
    ).astype(jnp.bfloat16)

    positions = lax.broadcasted_iota(jnp.int32, (16, 1024), 1)
    scale = HEAD**-0.5

    def attend(s):
        q = by_seq[pl.ds(pl.multiple_of(s * 16, 16), 16), 0:HEAD]
        scores = jnp.dot(q, keys[s], preferred_element_type=jnp.float32) * scale
        scores = jnp.where(positions < lengths[half * 32 + s], scores, -jnp.inf)
        key_last = kv_own[0, pl.ds(half * 32 + s, 1), 0:HEAD]
        value_last = kv_own[1, pl.ds(half * 32 + s, 1), 0:HEAD]
        score_new = jnp.sum(q.astype(jnp.float32) * key_last, axis=1, keepdims=True) * scale
        score_max = jnp.maximum(jnp.max(scores, axis=1, keepdims=True), score_new)
        weights = jnp.exp(scores - score_max)
        weight_new = jnp.exp(score_new - score_max)
        denom = jnp.sum(weights, axis=1, keepdims=True) + weight_new
        mixed = lax.dot_general(
            weights.astype(jnp.bfloat16), values[s], both_last, preferred_element_type=jnp.float32
        )
        mixed = mixed + weight_new.astype(jnp.bfloat16).astype(jnp.float32) * value_last
        attended[pl.ds(pl.multiple_of(s * 16, 16), 16), 0:HEAD] = (mixed / denom).astype(jnp.bfloat16)

    attended[:, HEAD:LANES] = jnp.zeros((512, HEAD), jnp.bfloat16)
    for n in range(4):
        for which in range(2):
            cache_copy(which, n).wait()

        def attend_some(i, carry, n=n):
            for s in range(4):
                attend(n * 8 + i * 4 + s)
            return carry

        lax.fori_loop(0, 2, attend_some, 0)

    low = attended[...]
    high = pltpu.roll(low.astype(jnp.float32), HEAD, 1).astype(jnp.bfloat16)
    block = jnp.dot(to_head[0], low, preferred_element_type=jnp.float32)
    block = block + jnp.dot(to_head[1], high, preferred_element_type=jnp.float32)
    block = block.astype(jnp.bfloat16)

    colours = [Colour(place, heads[k], ORDERS[k], recv_in.at[k], send_in.at[k]) for k in range(3)]
    for k, (first, last) in enumerate(COLOURS):
        colour = colours[k]
        for u in range(first, last):
            heads[k][colour.c, colour.b, colour.a, u - first] = block[u * TILE_ROWS : (u + 1) * TILE_ROWS]

    w_mine, w_theirs = w_all.at[:, core], w_all.at[:, 1 - core]

    def share_w():
        w_arrived = w_all.at[pl.ds(0, CHIPS - 1), core]
        remote(w_arrived, w_arrived, w_sems.at[0], w_sems.at[1], place.sibling()).wait()
        own_w.wait()
        remote(w_mine, w_mine, w_sems.at[2], w_sems.at[3], place.sibling()).start()

    def nothing():
        pass

    fillers = [functools.partial(new_block, which, n) for n in range(1, 4) for which in range(2)]
    gather(colours, [nothing] * 2 + fillers + [nothing] * 2 + [share_w])
    remote(w_mine, w_theirs, w_sems.at[2], w_sems.at[3], place.sibling()).wait()

    for n in range(RING):
        residual_copy(n).wait()
    total[...] = residual[...].astype(jnp.float32)

    def tile(z, y, x, u):
        k = next(k for k, (first, last) in enumerate(COLOURS) if first <= u < last)
        at = {"z": z, "y": y, "x": x}
        a, b, c = (at[axis] for axis in ORDERS[k])
        return heads[k][c, b, a, u - COLOURS[k][0]]

    def group_step(g, carry):
        rows = [
            jnp.concatenate([tile(g // 2, g % 2 * 2 + y, x, j * 2 + i) for j in range(8)], axis=1)
            for x in range(RING)
            for y in range(2)
            for i in range(2)
        ]
        lhs = jnp.concatenate(rows, axis=0)
        rhs = w_all[pl.ds(g * 8, 8)].reshape(8 * LANES, LANES)
        total[...] += jnp.dot(lhs, rhs, preferred_element_type=jnp.float32)
        return carry

    lax.fori_loop(0, 8, group_step, 0)

    out_colours = [
        Colour(place, outs[k].at[core], ORDERS[k], recv_out.at[k], send_out.at[k], share.at[k]) for k in range(3)
    ]
    for k, (first, last) in enumerate(COLOURS):
        colour = out_colours[k]
        for u in range(first, last):
            outs[k][core, colour.c, colour.b, colour.a, u - first] = total[
                u * TILE_ROWS : (u + 1) * TILE_ROWS, :
            ].astype(jnp.bfloat16)
    for colour in colours:
        colour.close()
    gather(out_colours)
    for k, colour in enumerate(out_colours):
        colour.close()
        colour.close_share(outs[k].at[1 - core])


def whole_step(*args):
    held = [(RING, RING, RING, last - first, TILE_ROWS, LANES) for first, last in COLOURS]
    vmem, hbm = pl.BlockSpec(memory_space=pltpu.VMEM), pl.BlockSpec(memory_space=pl.ANY)
    return pl.pallas_call(
        step_kernel,
        out_shape=[jax.ShapeDtypeStruct((2, *shape), jnp.bfloat16) for shape in held]
        + [jax.ShapeDtypeStruct((64, 512), jnp.bfloat16)] * 2,
        in_specs=[hbm] * 7 + [pl.BlockSpec(memory_space=pltpu.SMEM)],
        out_specs=[vmem] * 5,
        scratch_shapes=[pltpu.VMEM(shape, jnp.bfloat16) for shape in held]
        + [
            pltpu.VMEM((CHIPS, 2, 64, LANES), jnp.bfloat16),
            pltpu.VMEM((8, 512, 1024), jnp.bfloat16),
            pltpu.VMEM((64, 8192), jnp.bfloat16),
            pltpu.VMEM((2, 4, 8192, LANES), jnp.bfloat16),
            pltpu.VMEM((32, HEAD, 1024), jnp.bfloat16),
            pltpu.VMEM((32, HEAD, 1024), jnp.bfloat16),
            pltpu.VMEM((512, LANES), jnp.bfloat16),
            pltpu.VMEM((16, 32, LANES), jnp.bfloat16),
            pltpu.VMEM((512, LANES), jnp.bfloat16),
            pltpu.VMEM((512, LANES), jnp.bfloat16),
            pltpu.VMEM((512, 512), jnp.bfloat16),
            pltpu.VMEM((2, 256, 512), jnp.bfloat16),
            pltpu.VMEM((2, 64, LANES), jnp.float32),
            pltpu.VMEM((256, LANES), jnp.float32),
            pltpu.VMEM((256, LANES), jnp.bfloat16),
            pltpu.SemaphoreType.DMA((3, 3, 3, 4)),
            pltpu.SemaphoreType.DMA((3, 3)),
            pltpu.SemaphoreType.DMA((3, 3, 3, 4)),
            pltpu.SemaphoreType.DMA((3, 3)),
            pltpu.SemaphoreType.DMA((3, 2)),
            pltpu.SemaphoreType.DMA((4,)),
            pltpu.SemaphoreType.DMA((2,)),
            pltpu.SemaphoreType.DMA((30,)),
        ],
        compiler_params=pltpu.CompilerParams(collective_id=0, has_side_effects=True, vmem_limit_bytes=52 << 20),
        name="whole_step",
    )(*args)


def lay_out_kernel(*refs):
    held, (out, rows, sems) = refs[:3], refs[3:]
    copies = []
    for n in range(RING):
        for core in range(2):
            block = n * 2 + core
            for i in range(4):
                u = n * 4 + i
                k = next(k for k, (first, last) in enumerate(COLOURS) if first <= u < last)
                for chip in range(CHIPS):
                    at = {"z": chip // 16, "y": chip // 4 % 4, "x": chip % 4}
                    a, b, c = (at[axis] for axis in ORDERS[k])
                    rows[block, i * TILE_ROWS : (i + 1) * TILE_ROWS, chip * LANES : (chip + 1) * LANES] = held[k][
                        core, c, b, a, u - COLOURS[k][0]
                    ]
            copy = pltpu.make_async_copy(rows.at[block], out.at[pl.ds(block * 64, 64)], sems.at[block])
            copy.start()
            copies.append(copy)
    for copy in copies:
        copy.wait()


def lay_out(held):
    vmem = pl.BlockSpec(memory_space=pltpu.VMEM)
    return pl.pallas_call(
        lay_out_kernel,
        out_shape=jax.ShapeDtypeStruct((512, CHIPS * LANES), jnp.bfloat16),
        in_specs=[vmem] * 3,
        out_specs=pl.BlockSpec(memory_space=pl.ANY),
        scratch_shapes=[pltpu.VMEM((8, 64, CHIPS * LANES), jnp.bfloat16), pltpu.SemaphoreType.DMA((8,))],
        compiler_params=pltpu.CompilerParams(vmem_limit_bytes=30 << 20),
        name="lay_out",
    )(*held)


def solution(mesh):
    def local_step(tokens, w_query, w_key, w_value, w_out, key_cache, value_cache, lengths):
        *held, key_new, value_new = whole_step(
            tokens,
            w_query.T,
            w_key,
            w_value,
            w_out,
            jnp.swapaxes(key_cache, 2, 3),
            jnp.swapaxes(value_cache, 2, 3),
            lengths,
        )
        return (lay_out(held), key_new.reshape(64, 8, HEAD), value_new.reshape(64, 8, HEAD))

    cache_spec = P(("replica", "model"), None, None, None)
    new_spec = P(("replica", "model"), None, None)
    return jax.shard_map(
        local_step,
        mesh=mesh,
        in_specs=(P("replica", None), P(None, ("heads", "model")), P(None, None), P(None, None), P(("heads", "model"), None), cache_spec, cache_spec, P(("replica", "model"))),
        out_specs=(P("replica", None), new_spec, new_spec),
        check_vma=False,
    )
```

```python
import functools

import jax
import jax.numpy as jnp
from jax import lax
from jax.experimental import pallas as pl
from jax.experimental.pallas import tpu as pltpu
from jax.sharding import PartitionSpec as P

MESH = pl.DeviceIdType.MESH
RING = 4
CHIPS = RING**3
HEAD = 64
TILE_ROWS, LANES = 16, 128
UNITS = 16
COLOURS = ((0, 5), (5, 10), (10, 16))
ORDERS = (("x", "y", "z"), ("y", "z", "x"), ("z", "x", "y"))
STEPS = (1, 3, 2)
SOURCES = (0, 3, 1, 2)


class Place:
    def __init__(self):
        heads, model = lax.axis_index("heads"), lax.axis_index("model")
        self.at = {"z": heads // RING, "y": heads % RING, "x": model // 2}
        self.core = model % 2
        self.ring = {axis: [(at + n) % RING for n in range(RING)] for axis, at in self.at.items()}

    def device(self, at, core):
        return (0, at["z"] * RING + at["y"], at["x"] * 2 + core)

    def along(self, axis, step):
        at = dict(self.at)
        at[axis] = self.ring[axis][step]
        return self.device(at, self.core)

    def sibling(self):
        return self.device(self.at, 1 - self.core)

    def chip(self):
        return (self.at["z"] * RING + self.at["y"]) * RING + self.at["x"]

    def others(self):
        for n in range(1, CHIPS):
            z, y, x = n // 16, n // 4 % 4, n % 4
            at = {"z": self.ring["z"][z], "y": self.ring["y"][y], "x": self.ring["x"][x]}
            yield self.device(at, self.core), (at["z"] * RING + at["y"]) * RING + at["x"]


def remote(src, dst, send_sem, recv_sem, device):
    return pltpu.make_async_remote_copy(
        src_ref=src, dst_ref=dst, send_sem=send_sem, recv_sem=recv_sem, device_id=device, device_id_type=MESH
    )


def order_of(k, core):
    return ORDERS[(k + core) % 3]


def by_core(core, first, second):
    return first + core * (second - first)


LINE, NEAR, FAR, PLANE, FAR_PLANE = (0, 16), (3, 32), (7, 16), (11, 32), (27, 64)
RECV_COUNT = 31


class Colour:
    def __init__(self, place, held, k, own, recv, send, share=None):
        self.held, self.own, self.recv, self.send, self.share = held, own, recv, send, share
        orders = [order_of(k, core) for core in range(2)]
        self.a, self.b, self.c = (by_core(place.core, place.at[p], place.at[q]) for p, q in zip(*orders))
        self.sibling = place.sibling()
        self.ring = []
        for p, q in zip(*orders):
            to = {}
            for step in STEPS:
                first, second = place.along(p, step), place.along(q, step)
                to[step] = tuple(by_core(place.core, i, j) for i, j in zip(first, second))
            self.ring.append(to)
        self.as_ = [(self.a + n) % RING for n in range(RING)]
        self.bs = [(self.b + n) % RING for n in range(RING)]
        self.cs = [(self.c + n) % RING for n in range(RING)]

    def piece(self, plane, row, t):
        return self.held.at[self.cs[plane], self.bs[row], self.as_[SOURCES[t]]]

    def row(self, plane, n):
        return self.held.at[self.cs[plane], self.bs[n]]

    def copy(self, ref, phase, kind, index, step, source=None):
        source = ref if source is None else source
        return remote(source, ref, self.send.at[phase], self.recv.at[kind[0] + index], self.ring[phase][step])

    def along_b(self, ref, t, source=None):
        self.copy(ref, 1, NEAR, t, 1, source).start()
        self.copy(ref, 1, NEAR, t, 3, source).start()

    def along_c(self, ref, n, t, source=None):
        self.copy(ref, 2, PLANE, n * 4 + t, 1, source).start()
        self.copy(ref, 2, PLANE, n * 4 + t, 3, source).start()

    def give(self, ref, source=None):
        if self.share is not None:
            source = ref if source is None else source
            remote(source, ref, self.share.at[0], self.share.at[1], self.sibling).start()

    def open(self):
        own = self.piece(0, 0, 0)
        for slot, step in enumerate(STEPS):
            self.copy(own, 0, LINE, slot, step, self.own).start()
        self.along_b(own, 0, self.own)
        self.along_c(own, 0, 0, self.own)
        self.give(own, self.own)

    def line(self, t):
        ref = self.piece(0, 0, t)
        self.along_b(ref, t)
        self.give(ref)

    def line_on(self, t):
        self.along_c(self.piece(0, 0, t), 0, t)

    def near(self, t):
        slot, row, step = (0, 3, 1) if t in (0, 3) else (1, 1, 3)
        self.copy(self.piece(0, row, t), 1, FAR, t, step).start()

    def near_on(self, t):
        for slot, row in enumerate((3, 1)):
            self.along_c(self.piece(0, row, t), 1 + slot, t)
            if t == 3:
                self.give(self.row(0, row))

    def far(self, t):
        self.along_c(self.piece(0, 2, t), 3, t)
        if t == 3:
            self.give(self.row(0, 2))

    def plane(self, n, t):
        plane, step = (3, 1) if t in (0, 3) else (1, 3)
        self.copy(self.piece(plane, SOURCES[n], t), 2, FAR_PLANE, n, step).start()
        if t == 3:
            for plane in (3, 1):
                self.give(self.row(plane, SOURCES[n]))

    def far_plane(self, n):
        self.give(self.row(2, SOURCES[n]))

    def close(self):
        for ref, phase in ((self.held.at[0, 0, 0:3], 0), (self.held.at[0, 0:3], 1), (self.held.at[0:3], 2)):
            remote(ref, ref, self.send.at[phase], self.recv.at[0], self.sibling).wait_send()

    def close_share(self, other):
        remote(self.held, other, self.share.at[0], self.share.at[1], self.sibling).wait()


GATHER = [("open",)]
GATHER += [("line", t) for t in range(1, RING)]
GATHER += [("line_on", t) for t in range(1, RING)]
for _t in range(RING):
    GATHER += [("near", _t), ("near_on", _t), ("plane", 0, _t)]
for _t in range(RING):
    GATHER += [("far", _t), ("plane", 1, _t), ("plane", 2, _t)]
GATHER += [("plane", 3, _t) for _t in range(RING)]
GATHER += [("far_plane", _n) for _n in range(RING)]


def gather(colours, tiles, fillers=None):
    fillers = fillers or {}
    first = colours[0]

    def wait(kind, index):
        ref = tiles(kind[1])
        remote(ref, ref, first.send.at[0], first.recv.at[kind[0] + index], first.sibling).wait_recv()

    for step in GATHER:
        if step[0] == "line":
            wait(LINE, step[1] - 1)
        elif step[0] == "near":
            wait(NEAR, step[1])
        elif step[0] == "far":
            wait(FAR, step[1])
        elif step[0] == "plane":
            wait(PLANE, step[1] * 4 + step[2])
        elif step[0] == "far_plane":
            wait(FAR_PLANE, step[1])
        for colour in colours:
            getattr(colour, step[0])(*step[1:])
        for filler in fillers.get(step, ()):
            filler()


def step_kernel(
    tokens, w_query, w_key, w_value, w_out_hbm, key_cache, value_cache, lengths_hbm,
    out_a, out_b, out_c, own_out, key_new, value_new,
    head_a, head_b, head_c, w_all, w_out, tok, wq, w_kv, keys, values, query, by_head, by_seq,
    attended, to_seq, to_head, kv_own, total, residual, lengths,
    recv_in, send_in, recv_out, send_out, share, w_sems, q_sems, local_sems,
):
    outs, heads = (out_a, out_b, out_c), (head_a, head_b, head_c)
    place = Place()
    chip, core = place.chip(), place.core
    head_at, model_at = lax.axis_index("heads"), lax.axis_index("model")
    group, half = head_at // 2, head_at % 2
    barrier = pltpu.get_barrier_semaphore()

    halves = [half, 1 - half]
    models = [(model_at + n) % 8 for n in range(8)]

    def partner(n):
        other_half, other_model = halves[n // 8], models[n % 8]
        return (0, group * 2 + other_half, other_model), other_half, other_model

    def signal(device):
        pl.semaphore_signal(barrier, inc=1, device_id=device, device_id_type=MESH)

    def greet():
        for device, _ in place.others():
            signal(device)
        for n in range(RING):
            for other_half in range(2):
                signal((0, group * 2 + other_half, n * 2 + 1 - core))

    def token_copy(n):
        return pltpu.make_async_copy(tokens.at[:, pl.ds(n * 1024, 1024)], tok.at[n], local_sems.at[n])

    wq_copy = pltpu.make_async_copy(w_query, wq, local_sems.at[8])
    wq_copy.start()
    for n in range(8):
        token_copy(n).start()

    def kv_block(n):
        return (group // 2 + n) % 4

    def w_kv_copy(which, n):
        columns = pl.ds(pl.multiple_of(kv_block(n) * LANES, LANES), LANES)
        source = (w_key, w_value)[which]
        return pltpu.make_async_copy(source.at[:, columns], w_kv.at[which, n % 2], local_sems.at[9 + which * 4 + n])

    own_w = pltpu.make_async_copy(w_out_hbm, w_out, local_sems.at[29])
    own_w.start()
    for which in range(2):
        w_kv_copy(which, 0).start()

    def cache_copy(which, n):
        source, held = ((key_cache, keys), (value_cache, values))[which]
        return pltpu.make_async_copy(
            source.at[pl.ds(half * 32 + n * 8, 8), group], held.at[pl.ds(n * 8, 8)], local_sems.at[17 + which * 4 + n]
        )

    for n in range(4):
        for which in range(2):
            cache_copy(which, n).start()

    def residual_copy(n):
        rows = pl.ds(pl.multiple_of(n * 128 + core * 64, 64), 64)
        columns = pl.ds(pl.multiple_of(chip * LANES, LANES), LANES)
        return pltpu.make_async_copy(tokens.at[rows, columns], residual.at[pl.ds(n * 64, 64)], local_sems.at[25 + n])

    for n in range(RING):
        residual_copy(n).start()
    for which in range(2):
        w_kv_copy(which, 1).start()

    lengths_copy = pltpu.make_async_copy(lengths_hbm, lengths, local_sems.at[30])
    lengths_copy.start()
    greet()

    wq_copy.wait()
    token_copy(0).wait()
    both_last = (((1,), (1,)), ((), ()))

    def query_part(n):
        part = wq[:, n * 1024 : (n + 1) * 1024]
        return [
            lax.dot_general(tok[n, r : r + 256], part, both_last, preferred_element_type=jnp.float32) for r in (0, 256)
        ]

    acc = query_part(0)
    for n in range(1, 8):
        token_copy(n).wait()
        acc = [a + p for a, p in zip(acc, query_part(n))]
    for i, a in enumerate(acc):
        query[i * 256 : (i + 1) * 256, 0:HEAD] = a.astype(jnp.bfloat16)
    query[:, HEAD:LANES] = jnp.zeros((512, HEAD), jnp.bfloat16)

    pl.semaphore_wait(barrier, CHIPS - 1 + 2 * RING)
    slot = half * 8 + model_at

    def query_rows(other_half, other_model):
        return query.at[pl.ds(pl.multiple_of(other_model * 64 + other_half * 32, 32), 32)]

    for n in range(1, 16):
        device, other_half, other_model = partner(n)
        remote(query_rows(other_half, other_model), by_head.at[slot], q_sems.at[0], q_sems.at[1], device).start()

    own_w.wait()
    for device, target in place.others():
        columns = pl.ds(pl.multiple_of(target * LANES, LANES), LANES)
        remote(w_out.at[:, columns], w_all.at[chip, core], w_sems.at[0], w_sems.at[1], device).start()
    w_all[chip, core] = w_out[:, pl.ds(pl.multiple_of(chip * LANES, LANES), LANES)]
    by_head[slot] = query_rows(half, model_at)[...]

    own_rows = pl.ds(pl.multiple_of(model_at * 64, 64), 64)

    def new_block(which, n):
        w_kv_copy(which, n).wait()
        acc = jnp.dot(tok[0, own_rows], w_kv[which, n % 2, 0:1024], preferred_element_type=jnp.float32)
        for k in range(1, 8):
            acc = acc + jnp.dot(
                tok[k, own_rows], w_kv[which, n % 2, k * 1024 : (k + 1) * 1024], preferred_element_type=jnp.float32
            )
        if n < 2:
            w_kv_copy(which, n + 2).start()
        acc = acc.astype(jnp.bfloat16)
        columns = pl.ds(pl.multiple_of(kv_block(n) * LANES, LANES), LANES)
        (key_new, value_new)[which][:, columns] = acc
        if n == 0:
            wide = acc.astype(jnp.float32)
            wide = jnp.where(group % 2 == 0, wide, pltpu.roll(wide, HEAD, 1))
            lanes = lax.broadcasted_iota(jnp.int32, wide.shape, 1)
            kv_own[which] = jnp.where(lanes < HEAD, wide, 0.0)

    for which in range(2):
        new_block(which, 0)

    row = lax.broadcasted_iota(jnp.int32, (512, 512), 0)
    column = lax.broadcasted_iota(jnp.int32, (512, 512), 1)
    to_seq[...] = (column == (row % 16) * 32 + row // 16).astype(jnp.float32).astype(jnp.bfloat16)
    pair_row = lax.broadcasted_iota(jnp.int32, (256, 512), 0)
    pair_column = lax.broadcasted_iota(jnp.int32, (256, 512), 1)
    for parity in range(2):
        source = (pair_row % 32) * 16 + (pair_row // 32) * 2 + parity
        to_head[parity] = (pair_column == source).astype(jnp.float32).astype(jnp.bfloat16)

    lengths_copy.wait()
    arrived = by_head.at[pl.ds(0, 15)]
    remote(arrived, arrived, q_sems.at[0], q_sems.at[1], place.sibling()).wait()
    by_seq[...] = jnp.dot(
        to_seq[...], by_head[...].reshape(512, LANES), preferred_element_type=jnp.float32
    ).astype(jnp.bfloat16)

    positions = lax.broadcasted_iota(jnp.int32, (16, 1024), 1)
    scale = HEAD**-0.5

    def attend(s):
        q = by_seq[pl.ds(pl.multiple_of(s * 16, 16), 16), 0:HEAD]
        scores = jnp.dot(q, keys[s], preferred_element_type=jnp.float32) * scale
        scores = jnp.where(positions < lengths[half * 32 + s], scores, -jnp.inf)
        key_last = kv_own[0, pl.ds(half * 32 + s, 1), 0:HEAD]
        value_last = kv_own[1, pl.ds(half * 32 + s, 1), 0:HEAD]
        score_new = jnp.sum(q.astype(jnp.float32) * key_last, axis=1, keepdims=True) * scale
        score_max = jnp.maximum(jnp.max(scores, axis=1, keepdims=True), score_new)
        weights = jnp.exp(scores - score_max)
        weight_new = jnp.exp(score_new - score_max)
        denom = jnp.sum(weights, axis=1, keepdims=True) + weight_new
        mixed = lax.dot_general(
            weights.astype(jnp.bfloat16), values[s], both_last, preferred_element_type=jnp.float32
        )
        mixed = mixed + weight_new.astype(jnp.bfloat16).astype(jnp.float32) * value_last
        attended[pl.ds(pl.multiple_of(s * 16, 16), 16), 0:HEAD] = (mixed / denom).astype(jnp.bfloat16)

    attended[:, HEAD:LANES] = jnp.zeros((512, HEAD), jnp.bfloat16)
    for n in range(4):
        for which in range(2):
            cache_copy(which, n).wait()

        def attend_some(i, carry, n=n):
            for s in range(4):
                attend(n * 8 + i * 4 + s)
            return carry

        lax.fori_loop(0, 2, attend_some, 0)

    low = attended[...]
    high = pltpu.roll(low.astype(jnp.float32), HEAD, 1).astype(jnp.bfloat16)
    block = jnp.dot(to_head[0], low, preferred_element_type=jnp.float32)
    block = block + jnp.dot(to_head[1], high, preferred_element_type=jnp.float32)
    block = block.astype(jnp.bfloat16)

    colours = [Colour(place, heads[k], k, None, recv_in, send_in.at[k]) for k in range(3)]
    for k, (first, last) in enumerate(COLOURS):
        colour = colours[k]
        for u in range(first, last):
            heads[k][colour.c, colour.b, colour.a, u - first] = block[u * TILE_ROWS : (u + 1) * TILE_ROWS]

    w_mine, w_theirs = w_all.at[:, core], w_all.at[:, 1 - core]

    def share_w():
        w_arrived = w_all.at[pl.ds(0, CHIPS - 1), core]
        remote(w_arrived, w_arrived, w_sems.at[0], w_sems.at[1], place.sibling()).wait()
        remote(w_mine, w_mine, w_sems.at[2], w_sems.at[3], place.sibling()).start()

    new_blocks = [functools.partial(new_block, which, n) for n in range(1, 4) for which in range(2)]
    def tiles(n):
        return tok.at[0, pl.ds(0, n * 2)]

    gather(colours, tiles, {("open",): new_blocks, ("plane", 2, 3): [share_w]})
    remote(w_mine, w_theirs, w_sems.at[2], w_sems.at[3], place.sibling()).wait()

    for n in range(RING):
        residual_copy(n).wait()
    total[...] = residual[...].astype(jnp.float32)

    def tile(z, y, x, u):
        k = next(k for k, (first, last) in enumerate(COLOURS) if first <= u < last)
        at = {"z": z, "y": y, "x": x}
        a, b, c = (by_core(core, at[p], at[q]) for p, q in zip(order_of(k, 0), order_of(k, 1)))
        return heads[k][c, b, a, u - COLOURS[k][0]]

    def group_step(g, carry):
        rows = [
            jnp.concatenate([tile(g // 2, g % 2 * 2 + y, x, j * 2 + i) for j in range(8)], axis=1)
            for x in range(RING)
            for y in range(2)
            for i in range(2)
        ]
        rhs = w_all[pl.ds(g * 8, 8)].reshape(8 * LANES, LANES)
        parts = [
            jnp.dot(jnp.concatenate(rows[n : n + 8], axis=0), rhs, preferred_element_type=jnp.float32) for n in (0, 8)
        ]
        for n, part in enumerate(parts):
            total[n * 128 : (n + 1) * 128] += part
        return carry

    lax.fori_loop(0, 8, group_step, 0)

    out_colours = [
        Colour(place, outs[k].at[core], k, own_out.at[first:last], recv_out, send_out.at[k], share.at[k])
        for k, (first, last) in enumerate(COLOURS)
    ]
    for u in range(UNITS):
        own_out[u] = total[u * TILE_ROWS : (u + 1) * TILE_ROWS, :].astype(jnp.bfloat16)
    for colour in colours:
        colour.close()
    gather(out_colours, tiles)
    for k, colour in enumerate(out_colours):
        colour.close()
        colour.close_share(outs[k].at[1 - core])


def whole_step(*args):
    held = [(RING, RING, RING, last - first, TILE_ROWS, LANES) for first, last in COLOURS]
    vmem, hbm = pl.BlockSpec(memory_space=pltpu.VMEM), pl.BlockSpec(memory_space=pltpu.HBM)
    return pl.pallas_call(
        step_kernel,
        out_shape=[pltpu.VMEM((2, *shape), jnp.bfloat16) for shape in held]
        + [jax.ShapeDtypeStruct((UNITS, TILE_ROWS, LANES), jnp.bfloat16)]
        + [jax.ShapeDtypeStruct((64, 512), jnp.bfloat16)] * 2,
        in_specs=[hbm] * 8,
        out_specs=[pl.BlockSpec(memory_space=pl.ANY)] * 3 + [vmem] * 3,
        scratch_shapes=[pltpu.VMEM(shape, jnp.bfloat16) for shape in held]
        + [
            pltpu.VMEM((CHIPS, 2, 64, LANES), jnp.bfloat16),
            pltpu.VMEM((64, 8192), jnp.bfloat16),
            pltpu.VMEM((8, 512, 1024), jnp.bfloat16),
            pltpu.VMEM((64, 8192), jnp.bfloat16),
            pltpu.VMEM((2, 2, 8192, LANES), jnp.bfloat16),
            pltpu.VMEM((32, HEAD, 1024), jnp.bfloat16),
            pltpu.VMEM((32, HEAD, 1024), jnp.bfloat16),
            pltpu.VMEM((512, LANES), jnp.bfloat16),
            pltpu.VMEM((16, 32, LANES), jnp.bfloat16),
            pltpu.VMEM((512, LANES), jnp.bfloat16),
            pltpu.VMEM((512, LANES), jnp.bfloat16),
            pltpu.VMEM((512, 512), jnp.bfloat16),
            pltpu.VMEM((2, 256, 512), jnp.bfloat16),
            pltpu.VMEM((2, 64, LANES), jnp.float32),
            pltpu.VMEM((256, LANES), jnp.float32),
            pltpu.VMEM((256, LANES), jnp.bfloat16),
            pltpu.SMEM((64,), jnp.int32),
            pltpu.SemaphoreType.DMA((RECV_COUNT,)),
            pltpu.SemaphoreType.DMA((3, 3)),
            pltpu.SemaphoreType.DMA((RECV_COUNT,)),
            pltpu.SemaphoreType.DMA((3, 3)),
            pltpu.SemaphoreType.DMA((3, 2)),
            pltpu.SemaphoreType.DMA((4,)),
            pltpu.SemaphoreType.DMA((2,)),
            pltpu.SemaphoreType.DMA((31,)),
        ],
        compiler_params=pltpu.CompilerParams(collective_id=0, has_side_effects=True, vmem_limit_bytes=42 << 20),
        name="whole_step",
    )(*args)


def lay_out_kernel(*refs):
    held, own, news, (out, key_out, value_out, rows, new_rows, sems) = refs[:3], refs[3], refs[4:6], refs[6:]
    place = Place()
    own_columns = pl.ds(pl.multiple_of(place.chip() * LANES, LANES), LANES)
    copies = []
    for n in range(RING):
        for core in range(2):
            block = n * 2 + core
            for i in range(4):
                u = n * 4 + i
                k = next(k for k, (first, last) in enumerate(COLOURS) if first <= u < last)
                for chip in range(CHIPS):
                    at = {"z": chip // 16, "y": chip // 4 % 4, "x": chip % 4}
                    a, b, c = (at[axis] for axis in order_of(k, core))
                    rows[block, i * TILE_ROWS : (i + 1) * TILE_ROWS, chip * LANES : (chip + 1) * LANES] = held[k][
                        core, c, b, a, u - COLOURS[k][0]
                    ]

            @pl.when(place.core == core)
            def _(n=n, block=block):
                for i in range(4):
                    rows[block, i * TILE_ROWS : (i + 1) * TILE_ROWS, own_columns] = own[n * 4 + i]

            copy = pltpu.make_async_copy(rows.at[block], out.at[pl.ds(block * 64, 64)], sems.at[block])
            copy.start()
            copies.append(copy)
    for which, target in enumerate((key_out, value_out)):
        wide = news[which][...].astype(jnp.float32)
        parts = [wide[:, g * HEAD : (g + 1) * HEAD] for g in range(8)]
        new_rows[which] = jnp.stack(parts, axis=1).astype(jnp.bfloat16)
        copy = pltpu.make_async_copy(new_rows.at[which], target, sems.at[8 + which])
        copy.start()
        copies.append(copy)
    for copy in copies:
        copy.wait()


def lay_out(*held):
    vmem = pl.BlockSpec(memory_space=pltpu.VMEM)
    return pl.pallas_call(
        lay_out_kernel,
        out_shape=[jax.ShapeDtypeStruct((512, CHIPS * LANES), jnp.bfloat16)]
        + [jax.ShapeDtypeStruct((64, 8, HEAD), jnp.bfloat16)] * 2,
        in_specs=[vmem] * 6,
        out_specs=[pl.BlockSpec(memory_space=pltpu.HBM)] * 3,
        scratch_shapes=[
            pltpu.VMEM((8, 64, CHIPS * LANES), jnp.bfloat16),
            pltpu.VMEM((2, 64, 8, HEAD), jnp.bfloat16),
            pltpu.SemaphoreType.DMA((10,)),
        ],
        compiler_params=pltpu.CompilerParams(vmem_limit_bytes=30 << 20),
        name="lay_out",
    )(*held)


def solution(mesh):
    def local_step(tokens, w_query, w_key, w_value, w_out, key_cache, value_cache, lengths):
        held = whole_step(
            tokens,
            pltpu.with_memory_space_constraint(w_query.T, pltpu.HBM),
            w_key,
            w_value,
            pltpu.with_memory_space_constraint(w_out, pltpu.HBM),
            jnp.swapaxes(key_cache, 2, 3),
            jnp.swapaxes(value_cache, 2, 3),
            pltpu.with_memory_space_constraint(lengths, pltpu.HBM),
        )
        return tuple(lay_out(*held))

    cache_spec = P(("replica", "model"), None, None, None)
    new_spec = P(("replica", "model"), None, None)
    return jax.shard_map(
        local_step,
        mesh=mesh,
        in_specs=(P("replica", None), P(None, ("heads", "model")), P(None, None), P(None, None), P(("heads", "model"), None), cache_spec, cache_spec, P(("replica", "model"))),
        out_specs=(P("replica", None), new_spec, new_spec),
        check_vma=False,
    )
```

```python
import functools

import jax
import jax.numpy as jnp
from jax import lax
from jax.experimental import pallas as pl
from jax.experimental.pallas import tpu as pltpu
from jax.sharding import PartitionSpec as P

MESH = pl.DeviceIdType.MESH
RING = 4
CHIPS = RING**3
STRIDE = 29
HEAD = 64
TILE_ROWS, LANES = 16, 128
UNITS = 16
COLOURS = ((0, 5), (5, 10), (10, 16))
ORDERS = (("x", "y", "z"), ("y", "z", "x"), ("z", "x", "y"))
STEPS = (1, 3, 2)
SOURCES = (0, 3, 1, 2)


class Place:
    def __init__(self):
        heads, model = lax.axis_index("heads"), lax.axis_index("model")
        self.at = {"z": heads // RING, "y": heads % RING, "x": model // 2}
        self.core = model % 2
        self.ring = {axis: [(at + n) % RING for n in range(RING)] for axis, at in self.at.items()}

    def device(self, at, core):
        return (0, at["z"] * RING + at["y"], at["x"] * 2 + core)

    def along(self, axis, step):
        at = dict(self.at)
        at[axis] = self.ring[axis][step]
        return self.device(at, self.core)

    def sibling(self):
        return self.device(self.at, 1 - self.core)

    def chip(self):
        return (self.at["z"] * RING + self.at["y"]) * RING + self.at["x"]

    def others(self):
        for i in range(1, CHIPS):
            n = i * STRIDE % CHIPS
            z, y, x = n // 16, n // 4 % 4, n % 4
            at = {"z": self.ring["z"][z], "y": self.ring["y"][y], "x": self.ring["x"][x]}
            yield self.device(at, self.core), (at["z"] * RING + at["y"]) * RING + at["x"]


def remote(src, dst, send_sem, recv_sem, device):
    return pltpu.make_async_remote_copy(
        src_ref=src, dst_ref=dst, send_sem=send_sem, recv_sem=recv_sem, device_id=device, device_id_type=MESH
    )


def order_of(k, core):
    return ORDERS[(k + core) % 3]


def by_core(core, first, second):
    return first + core * (second - first)


LINE, NEAR, FAR, PLANE, FAR_PLANE = (0, 16), (3, 32), (7, 16), (11, 32), (27, 64)
RECV_COUNT = 31
DIRECT = (2, 3)


class Colour:
    def __init__(self, place, held, k, own, recv, send, share=None):
        self.held, self.own, self.recv, self.send, self.share = held, own, recv, send, share
        orders = [order_of(k, core) for core in range(2)]
        self.a, self.b, self.c = (by_core(place.core, place.at[p], place.at[q]) for p, q in zip(*orders))
        self.sibling = place.sibling()
        self.ring = []
        for p, q in zip(*orders):
            to = {}
            for step in STEPS:
                first, second = place.along(p, step), place.along(q, step)
                to[step] = tuple(by_core(place.core, i, j) for i, j in zip(first, second))
            self.ring.append(to)
        self.as_ = [(self.a + n) % RING for n in range(RING)]
        self.bs = [(self.b + n) % RING for n in range(RING)]
        self.cs = [(self.c + n) % RING for n in range(RING)]

    def piece(self, plane, row, t):
        return self.held.at[self.cs[plane], self.bs[row], self.as_[SOURCES[t]]]

    def row(self, plane, n):
        return self.held.at[self.cs[plane], self.bs[n]]

    def copy(self, ref, phase, kind, index, step, source=None):
        source = ref if source is None else source
        return remote(source, ref, self.send.at[phase], self.recv.at[kind[0] + index], self.ring[phase][step])

    def along_b(self, ref, t, source=None):
        self.copy(ref, 1, NEAR, t, 1, source).start()
        self.copy(ref, 1, NEAR, t, 3, source).start()

    def along_c(self, ref, n, t, source=None):
        self.copy(ref, 2, PLANE, n * 4 + t, 1, source).start()
        self.copy(ref, 2, PLANE, n * 4 + t, 3, source).start()

    def give(self, ref, source=None):
        if self.share is not None:
            source = ref if source is None else source
            remote(source, ref, self.share.at[0], self.share.at[1], self.sibling).start()

    def open(self):
        own = self.piece(0, 0, 0)
        for slot, step in enumerate(STEPS):
            self.copy(own, 0, LINE, slot, step, self.own).start()

    def open_b(self):
        self.along_b(self.piece(0, 0, 0), 0, self.own)

    def open_c(self):
        self.along_c(self.piece(0, 0, 0), 0, 0, self.own)
        self.give(self.piece(0, 0, 0), self.own)

    def line(self, t):
        ref = self.piece(0, 0, t)
        self.along_b(ref, t)
        self.give(ref)

    def line_on(self, t):
        self.along_c(self.piece(0, 0, t), 0, t)

    def near(self, t):
        slot, row, step = (0, 3, 1) if t in (0, 3) else (1, 1, 3)
        self.copy(self.piece(0, row, t), 1, FAR, t, step).start()

    def near_on(self, t):
        for slot, row in enumerate((3, 1)):
            self.along_c(self.piece(0, row, t), 1 + slot, t)
            if t == 3:
                self.give(self.row(0, row))

    def far(self, t):
        self.along_c(self.piece(0, 2, t), 3, t)
        if t in DIRECT:
            self.copy(self.piece(0, 2, t), 2, FAR_PLANE, 3, 2).start()
        if t == 3:
            self.give(self.row(0, 2))

    def plane(self, n, t):
        plane, step = (3, 1) if t in (0, 3) else (1, 3)
        if n < 3 or t not in DIRECT:
            self.copy(self.piece(plane, SOURCES[n], t), 2, FAR_PLANE, n, step).start()
        if t == 3:
            for plane in (3, 1):
                self.give(self.row(plane, SOURCES[n]))

    def far_plane(self, n):
        self.give(self.row(2, SOURCES[n]))

    def close(self):
        for ref, phase in ((self.held.at[0, 0, 0:3], 0), (self.held.at[0, 0:3], 1), (self.held.at[0:3], 2)):
            remote(ref, ref, self.send.at[phase], self.recv.at[0], self.sibling).wait_send()

    def close_share(self, other):
        remote(self.held, other, self.share.at[0], self.share.at[1], self.sibling).wait()


GATHER = [("open",), ("open_b",), ("open_c",)]
GATHER += [("line", t) for t in range(1, RING)]
GATHER += [("line_on", t) for t in range(1, RING)]
for _t in range(RING):
    GATHER += [("near", _t), ("near_on", _t)]
for _t in range(RING):
    GATHER += [("plane", 0, _t), ("far", _t)]
for _t in range(RING):
    GATHER += [("plane", 1, _t), ("plane", 2, _t)]
GATHER += [("plane", 3, _t) for _t in range(RING)]
GATHER += [("far_plane", _n) for _n in range(RING)]


def gather(colours, tiles, fillers=None):
    fillers = fillers or {}
    first = colours[0]

    def wait(kind, index):
        ref = tiles(kind[1])
        remote(ref, ref, first.send.at[0], first.recv.at[kind[0] + index], first.sibling).wait_recv()

    for step in GATHER:
        if step[0] == "line":
            wait(LINE, step[1] - 1)
        elif step[0] == "near":
            wait(NEAR, step[1])
        elif step[0] == "far":
            wait(FAR, step[1])
        elif step[0] == "plane":
            wait(PLANE, step[1] * 4 + step[2])
        elif step[0] == "far_plane":
            wait(FAR_PLANE, step[1])
        for colour in colours:
            getattr(colour, step[0])(*step[1:])
        for filler in fillers.get(step, ()):
            filler()


def step_kernel(
    tokens, w_query, w_key, w_value, w_out_hbm, key_cache, value_cache, lengths_hbm,
    out_a, out_b, out_c, own_out, key_new, value_new,
    head_a, head_b, head_c, w_all, w_out, tok, wq, w_kv, keys, values, query, by_head, by_seq,
    attended, to_seq, to_head, kv_own, total, residual, lengths,
    recv_in, send_in, recv_out, send_out, share, w_sems, q_sems, local_sems,
):
    outs, heads = (out_a, out_b, out_c), (head_a, head_b, head_c)
    place = Place()
    chip, core = place.chip(), place.core
    head_at, model_at = lax.axis_index("heads"), lax.axis_index("model")
    group, half = head_at // 2, head_at % 2
    barrier = pltpu.get_barrier_semaphore()

    halves = [half, 1 - half]
    models = [(model_at + n) % 8 for n in range(8)]

    def partner(n):
        other_half, other_model = halves[n // 8], models[n % 8]
        return (0, group * 2 + other_half, other_model), other_half, other_model

    def signal(device):
        pl.semaphore_signal(barrier, inc=1, device_id=device, device_id_type=MESH)

    def greet():
        for device, _ in place.others():
            signal(device)
        for n in range(RING):
            for other_half in range(2):
                signal((0, group * 2 + other_half, n * 2 + 1 - core))

    def token_copy(n):
        return pltpu.make_async_copy(tokens.at[:, pl.ds(n * 1024, 1024)], tok.at[n], local_sems.at[n])

    wq_copy = pltpu.make_async_copy(w_query, wq, local_sems.at[8])
    wq_copy.start()
    for n in range(8):
        token_copy(n).start()

    def kv_block(n):
        return (group // 2 + n) % 4

    def w_kv_copy(which, n):
        columns = pl.ds(pl.multiple_of(kv_block(n) * LANES, LANES), LANES)
        source = (w_key, w_value)[which]
        return pltpu.make_async_copy(source.at[:, columns], w_kv.at[which, n % 2], local_sems.at[9 + which * 4 + n])

    own_w = pltpu.make_async_copy(w_out_hbm, w_out, local_sems.at[29])
    own_w.start()
    for which in range(2):
        w_kv_copy(which, 0).start()

    def cache_copy(which, n):
        source, held = ((key_cache, keys), (value_cache, values))[which]
        return pltpu.make_async_copy(
            source.at[pl.ds(half * 32 + n * 8, 8), group], held.at[pl.ds(n * 8, 8)], local_sems.at[17 + which * 4 + n]
        )

    for n in range(4):
        for which in range(2):
            cache_copy(which, n).start()

    def residual_copy(n):
        rows = pl.ds(pl.multiple_of(n * 128 + core * 64, 64), 64)
        columns = pl.ds(pl.multiple_of(chip * LANES, LANES), LANES)
        return pltpu.make_async_copy(tokens.at[rows, columns], residual.at[pl.ds(n * 64, 64)], local_sems.at[25 + n])

    for n in range(RING):
        residual_copy(n).start()
    for which in range(2):
        w_kv_copy(which, 1).start()

    lengths_copy = pltpu.make_async_copy(lengths_hbm, lengths, local_sems.at[30])
    lengths_copy.start()
    greet()

    wq_copy.wait()
    token_copy(0).wait()
    both_last = (((1,), (1,)), ((), ()))

    def query_part(n):
        part = wq[:, n * 1024 : (n + 1) * 1024]
        return [
            lax.dot_general(tok[n, r : r + 256], part, both_last, preferred_element_type=jnp.float32) for r in (0, 256)
        ]

    acc = query_part(0)
    for n in range(1, 8):
        token_copy(n).wait()
        acc = [a + p for a, p in zip(acc, query_part(n))]
    for i, a in enumerate(acc):
        query[i * 256 : (i + 1) * 256, 0:HEAD] = a.astype(jnp.bfloat16)
    query[:, HEAD:LANES] = jnp.zeros((512, HEAD), jnp.bfloat16)

    pl.semaphore_wait(barrier, CHIPS - 1 + 2 * RING)
    slot = half * 8 + model_at

    def query_rows(other_half, other_model):
        return query.at[pl.ds(pl.multiple_of(other_model * 64 + other_half * 32, 32), 32)]

    for n in range(1, 16):
        device, other_half, other_model = partner(n)
        remote(query_rows(other_half, other_model), by_head.at[slot], q_sems.at[0], q_sems.at[1], device).start()

    own_w.wait()
    for device, target in place.others():
        columns = pl.ds(pl.multiple_of(target * LANES, LANES), LANES)
        remote(w_out.at[:, columns], w_all.at[chip, core], w_sems.at[0], w_sems.at[1], device).start()
    w_all[chip, core] = w_out[:, pl.ds(pl.multiple_of(chip * LANES, LANES), LANES)]
    by_head[slot] = query_rows(half, model_at)[...]

    own_rows = pl.ds(pl.multiple_of(model_at * 64, 64), 64)

    def new_block(which, n):
        w_kv_copy(which, n).wait()
        acc = jnp.dot(tok[0, own_rows], w_kv[which, n % 2, 0:1024], preferred_element_type=jnp.float32)
        for k in range(1, 8):
            acc = acc + jnp.dot(
                tok[k, own_rows], w_kv[which, n % 2, k * 1024 : (k + 1) * 1024], preferred_element_type=jnp.float32
            )
        if n < 2:
            w_kv_copy(which, n + 2).start()
        acc = acc.astype(jnp.bfloat16)
        columns = pl.ds(pl.multiple_of(kv_block(n) * LANES, LANES), LANES)
        (key_new, value_new)[which][:, columns] = acc
        if n == 0:
            wide = acc.astype(jnp.float32)
            wide = jnp.where(group % 2 == 0, wide, pltpu.roll(wide, HEAD, 1))
            lanes = lax.broadcasted_iota(jnp.int32, wide.shape, 1)
            kv_own[which] = jnp.where(lanes < HEAD, wide, 0.0)

    for which in range(2):
        new_block(which, 0)

    row = lax.broadcasted_iota(jnp.int32, (512, 512), 0)
    column = lax.broadcasted_iota(jnp.int32, (512, 512), 1)
    to_seq[...] = (column == (row % 16) * 32 + row // 16).astype(jnp.float32).astype(jnp.bfloat16)
    pair_row = lax.broadcasted_iota(jnp.int32, (256, 512), 0)
    pair_column = lax.broadcasted_iota(jnp.int32, (256, 512), 1)
    for parity in range(2):
        source = (pair_row % 32) * 16 + (pair_row // 32) * 2 + parity
        to_head[parity] = (pair_column == source).astype(jnp.float32).astype(jnp.bfloat16)

    lengths_copy.wait()
    arrived = by_head.at[pl.ds(0, 15)]
    remote(arrived, arrived, q_sems.at[0], q_sems.at[1], place.sibling()).wait()
    by_seq[...] = jnp.dot(
        to_seq[...], by_head[...].reshape(512, LANES), preferred_element_type=jnp.float32
    ).astype(jnp.bfloat16)

    positions = lax.broadcasted_iota(jnp.int32, (16, 1024), 1)
    scale = HEAD**-0.5

    def attend(s):
        q = by_seq[pl.ds(pl.multiple_of(s * 16, 16), 16), 0:HEAD]
        scores = jnp.dot(q, keys[s], preferred_element_type=jnp.float32) * scale
        scores = jnp.where(positions < lengths[half * 32 + s], scores, -jnp.inf)
        key_last = kv_own[0, pl.ds(half * 32 + s, 1), 0:HEAD]
        value_last = kv_own[1, pl.ds(half * 32 + s, 1), 0:HEAD]
        score_new = jnp.sum(q.astype(jnp.float32) * key_last, axis=1, keepdims=True) * scale
        score_max = jnp.maximum(jnp.max(scores, axis=1, keepdims=True), score_new)
        weights = jnp.exp(scores - score_max)
        weight_new = jnp.exp(score_new - score_max)
        denom = jnp.sum(weights, axis=1, keepdims=True) + weight_new
        mixed = lax.dot_general(
            weights.astype(jnp.bfloat16), values[s], both_last, preferred_element_type=jnp.float32
        )
        mixed = mixed + weight_new.astype(jnp.bfloat16).astype(jnp.float32) * value_last
        attended[pl.ds(pl.multiple_of(s * 16, 16), 16), 0:HEAD] = (mixed / denom).astype(jnp.bfloat16)

    attended[:, HEAD:LANES] = jnp.zeros((512, HEAD), jnp.bfloat16)
    for n in range(4):
        for which in range(2):
            cache_copy(which, n).wait()

        def attend_some(i, carry, n=n):
            for s in range(4):
                attend(n * 8 + i * 4 + s)
            return carry

        lax.fori_loop(0, 2, attend_some, 0)

    low = attended[...]
    high = pltpu.roll(low.astype(jnp.float32), HEAD, 1).astype(jnp.bfloat16)
    block = jnp.dot(to_head[0], low, preferred_element_type=jnp.float32)
    block = block + jnp.dot(to_head[1], high, preferred_element_type=jnp.float32)
    block = block.astype(jnp.bfloat16)

    colours = [Colour(place, heads[k], k, None, recv_in, send_in.at[k]) for k in range(3)]
    for k, (first, last) in enumerate(COLOURS):
        colour = colours[k]
        for u in range(first, last):
            heads[k][colour.c, colour.b, colour.a, u - first] = block[u * TILE_ROWS : (u + 1) * TILE_ROWS]

    w_mine, w_theirs = w_all.at[:, core], w_all.at[:, 1 - core]

    def share_w():
        w_arrived = w_all.at[pl.ds(0, CHIPS - 1), core]
        remote(w_arrived, w_arrived, w_sems.at[0], w_sems.at[1], place.sibling()).wait()
        remote(w_mine, w_mine, w_sems.at[2], w_sems.at[3], place.sibling()).start()

    new_blocks = [functools.partial(new_block, which, n) for n in range(1, 4) for which in range(2)]
    def tiles(n):
        return tok.at[0, pl.ds(0, n * 2)]

    gather(colours, tiles, {("open_c",): new_blocks, ("plane", 2, 3): [share_w]})
    remote(w_mine, w_theirs, w_sems.at[2], w_sems.at[3], place.sibling()).wait()

    for n in range(RING):
        residual_copy(n).wait()
    total[...] = residual[...].astype(jnp.float32)

    def tile(z, y, x, u):
        k = next(k for k, (first, last) in enumerate(COLOURS) if first <= u < last)
        at = {"z": z, "y": y, "x": x}
        a, b, c = (by_core(core, at[p], at[q]) for p, q in zip(order_of(k, 0), order_of(k, 1)))
        return heads[k][c, b, a, u - COLOURS[k][0]]

    def group_step(n, carry):
        parts = []
        for g in (n, n + 4):
            rows = [
                jnp.concatenate([tile(g // 2, g % 2 * 2 + y, x, j * 2 + i) for j in range(8)], axis=1)
                for x in range(RING)
                for y in range(2)
                for i in range(2)
            ]
            rhs = w_all[pl.ds(g * 8, 8)].reshape(8 * LANES, LANES)
            parts.append(jnp.dot(jnp.concatenate(rows, axis=0), rhs, preferred_element_type=jnp.float32))
        total[...] += parts[0] + parts[1]
        return carry

    lax.fori_loop(0, 4, group_step, 0)

    out_colours = [
        Colour(place, outs[k].at[core], k, own_out.at[first:last], recv_out, send_out.at[k], share.at[k])
        for k, (first, last) in enumerate(COLOURS)
    ]
    for u in range(UNITS):
        own_out[u] = total[u * TILE_ROWS : (u + 1) * TILE_ROWS, :].astype(jnp.bfloat16)
    for colour in colours:
        colour.close()
    gather(out_colours, tiles)
    for k, colour in enumerate(out_colours):
        colour.close()
        colour.close_share(outs[k].at[1 - core])


def whole_step(*args):
    held = [(RING, RING, RING, last - first, TILE_ROWS, LANES) for first, last in COLOURS]
    vmem, hbm = pl.BlockSpec(memory_space=pltpu.VMEM), pl.BlockSpec(memory_space=pltpu.HBM)
    return pl.pallas_call(
        step_kernel,
        out_shape=[pltpu.VMEM((2, *shape), jnp.bfloat16) for shape in held]
        + [jax.ShapeDtypeStruct((UNITS, TILE_ROWS, LANES), jnp.bfloat16)]
        + [jax.ShapeDtypeStruct((64, 512), jnp.bfloat16)] * 2,
        in_specs=[hbm] * 8,
        out_specs=[pl.BlockSpec(memory_space=pl.ANY)] * 3 + [vmem] * 3,
        scratch_shapes=[pltpu.VMEM(shape, jnp.bfloat16) for shape in held]
        + [
            pltpu.VMEM((CHIPS, 2, 64, LANES), jnp.bfloat16),
            pltpu.VMEM((64, 8192), jnp.bfloat16),
            pltpu.VMEM((8, 512, 1024), jnp.bfloat16),
            pltpu.VMEM((64, 8192), jnp.bfloat16),
            pltpu.VMEM((2, 2, 8192, LANES), jnp.bfloat16),
            pltpu.VMEM((32, HEAD, 1024), jnp.bfloat16),
            pltpu.VMEM((32, HEAD, 1024), jnp.bfloat16),
            pltpu.VMEM((512, LANES), jnp.bfloat16),
            pltpu.VMEM((16, 32, LANES), jnp.bfloat16),
            pltpu.VMEM((512, LANES), jnp.bfloat16),
            pltpu.VMEM((512, LANES), jnp.bfloat16),
            pltpu.VMEM((512, 512), jnp.bfloat16),
            pltpu.VMEM((2, 256, 512), jnp.bfloat16),
            pltpu.VMEM((2, 64, LANES), jnp.float32),
            pltpu.VMEM((256, LANES), jnp.float32),
            pltpu.VMEM((256, LANES), jnp.bfloat16),
            pltpu.SMEM((64,), jnp.int32),
            pltpu.SemaphoreType.DMA((RECV_COUNT,)),
            pltpu.SemaphoreType.DMA((3, 3)),
            pltpu.SemaphoreType.DMA((RECV_COUNT,)),
            pltpu.SemaphoreType.DMA((3, 3)),
            pltpu.SemaphoreType.DMA((3, 2)),
            pltpu.SemaphoreType.DMA((4,)),
            pltpu.SemaphoreType.DMA((2,)),
            pltpu.SemaphoreType.DMA((31,)),
        ],
        compiler_params=pltpu.CompilerParams(collective_id=0, has_side_effects=True, vmem_limit_bytes=42 << 20),
        name="whole_step",
    )(*args)


def lay_out_kernel(*refs):
    held, own, news, (out, key_out, value_out, rows, new_rows, sems) = refs[:3], refs[3], refs[4:6], refs[6:]
    place = Place()
    own_columns = pl.ds(pl.multiple_of(place.chip() * LANES, LANES), LANES)
    copies = []
    for n in range(RING):
        for core in range(2):
            block = n * 2 + core
            for i in range(4):
                u = n * 4 + i
                k = next(k for k, (first, last) in enumerate(COLOURS) if first <= u < last)
                for chip in range(CHIPS):
                    at = {"z": chip // 16, "y": chip // 4 % 4, "x": chip % 4}
                    a, b, c = (at[axis] for axis in order_of(k, core))
                    rows[block, i * TILE_ROWS : (i + 1) * TILE_ROWS, chip * LANES : (chip + 1) * LANES] = held[k][
                        core, c, b, a, u - COLOURS[k][0]
                    ]

            @pl.when(place.core == core)
            def _(n=n, block=block):
                for i in range(4):
                    rows[block, i * TILE_ROWS : (i + 1) * TILE_ROWS, own_columns] = own[n * 4 + i]

            copy = pltpu.make_async_copy(rows.at[block], out.at[pl.ds(block * 64, 64)], sems.at[block])
            copy.start()
            copies.append(copy)
    for which, target in enumerate((key_out, value_out)):
        wide = news[which][...].astype(jnp.float32)
        parts = [wide[:, g * HEAD : (g + 1) * HEAD] for g in range(8)]
        new_rows[which] = jnp.stack(parts, axis=1).astype(jnp.bfloat16)
        copy = pltpu.make_async_copy(new_rows.at[which], target, sems.at[8 + which])
        copy.start()
        copies.append(copy)
    for copy in copies:
        copy.wait()


def lay_out(*held):
    vmem = pl.BlockSpec(memory_space=pltpu.VMEM)
    return pl.pallas_call(
        lay_out_kernel,
        out_shape=[jax.ShapeDtypeStruct((512, CHIPS * LANES), jnp.bfloat16)]
        + [jax.ShapeDtypeStruct((64, 8, HEAD), jnp.bfloat16)] * 2,
        in_specs=[vmem] * 6,
        out_specs=[pl.BlockSpec(memory_space=pltpu.HBM)] * 3,
        scratch_shapes=[
            pltpu.VMEM((8, 64, CHIPS * LANES), jnp.bfloat16),
            pltpu.VMEM((2, 64, 8, HEAD), jnp.bfloat16),
            pltpu.SemaphoreType.DMA((10,)),
        ],
        compiler_params=pltpu.CompilerParams(vmem_limit_bytes=30 << 20),
        name="lay_out",
    )(*held)


def solution(mesh):
    def local_step(tokens, w_query, w_key, w_value, w_out, key_cache, value_cache, lengths):
        held = whole_step(
            tokens,
            pltpu.with_memory_space_constraint(w_query.T, pltpu.HBM),
            w_key,
            w_value,
            pltpu.with_memory_space_constraint(w_out, pltpu.HBM),
            jnp.swapaxes(key_cache, 2, 3),
            jnp.swapaxes(value_cache, 2, 3),
            pltpu.with_memory_space_constraint(lengths, pltpu.HBM),
        )
        return tuple(lay_out(*held))

    cache_spec = P(("replica", "model"), None, None, None)
    new_spec = P(("replica", "model"), None, None)
    return jax.shard_map(
        local_step,
        mesh=mesh,
        in_specs=(P("replica", None), P(None, ("heads", "model")), P(None, None), P(None, None), P(("heads", "model"), None), cache_spec, cache_spec, P(("replica", "model"))),
        out_specs=(P("replica", None), new_spec, new_spec),
        check_vma=False,
    )
```
